8 devices in a mesh: dp: 1 (over z), tp: 8 (over x, y, core).
Axes of the slice: x: 2, y: 2, z: 1, core: 2. Of those that a mesh axis runs over, the one named last changes fastest.
Arguments:
- x: bfloat16 [4096, 2048], P(('dp', 'tp'))
- w_gate: bfloat16 [2048, 8192], P(None, 'tp')
- w_up: bfloat16 [2048, 8192], P(None, 'tp')
- w_down: bfloat16 [8192, 2048], P('tp')
Outputs:
- output: bfloat16 [4096, 2048], P(('dp', 'tp'))
All inputs are finite; a program needn't handle non-finite values.
Results may differ from the reference program's by a relative error of at most 0.016.
Values are sent between devices in bfloat16 or wider.
A program may use at most 2 GiB of HBM per device.

```python
import jax
import jax.numpy as jnp

ROWS = 4096
D = 2048
FF = 8192


def setup_inputs(seed: int = 0, part: int = 0) -> dict:
    kx, kg, ku, kd = jax.random.split(jax.random.key(seed), 4)
    drawn = {
        "x": jax.random.normal(jax.random.fold_in(kx, part), (ROWS, D), jnp.float32),
        "w_gate": jax.random.normal(kg, (D, FF), jnp.float32) * D**-0.5,
        "w_up": jax.random.normal(ku, (D, FF), jnp.float32) * D**-0.5,
        "w_down": jax.random.normal(kd, (FF, D), jnp.float32) * FF**-0.5,
    }
    return {k: v.astype(jnp.bfloat16) for k, v in drawn.items()}


def reference(x, w_gate, w_up, w_down):
    gate = jnp.dot(x, w_gate, preferred_element_type=jnp.float32)
    up = jnp.dot(x, w_up, preferred_element_type=jnp.float32)
    hidden = (jax.nn.silu(gate) * up).astype(jnp.bfloat16)
    return jnp.dot(hidden, w_down, preferred_element_type=jnp.float32).astype(jnp.bfloat16)
```

```python
import jax
import jax.numpy as jnp
from jax import lax
from jax.experimental import pallas as pl
from jax.experimental.pallas import tpu as pltpu
from jax.sharding import PartitionSpec as P

BF16 = jnp.bfloat16
F32 = jnp.float32

SUB = 128
UNIT = 256
TILE = 256

OWN, BX, BY, BD = 0, 1, 2, 3


def kernel(
    x_hbm, wg_hbm, wu_hbm, wd_hbm, out_hbm,
    wg, wu, wd, xb, hid, pd, px, py, px32, py32, sx, sy, own, relx, rely, finx, finy, out,
    loc_sem, out_sem, w_send, w_recv, ag_send, ag_recv, fw_send, fw_recv, d_send, d_recv, f_send, f_recv,
):
    half = wg_hbm.shape[1]
    width = wd_hbm.shape[1]
    tiles = half // TILE

    me = lax.axis_index("tp")
    core = me % 2
    iy = (me // 2) % 2
    nx = (me + 4) % 8
    ny = me + 2 - 4 * iy
    sib = me + 1 - 2 * core

    local = [
        pltpu.make_async_copy(wg_hbm, wg.at[0], loc_sem.at[0]),
        pltpu.make_async_copy(wu_hbm, wu.at[0], loc_sem.at[1]),
        pltpu.make_async_copy(wd_hbm, wd.at[pl.ds(0, half)], loc_sem.at[2]),
        pltpu.make_async_copy(x_hbm, xb.at[OWN], loc_sem.at[3]),
    ]
    for c in local:
        c.start()

    barrier = pltpu.get_barrier_semaphore()
    for d in (nx, ny, sib):
        pl.semaphore_signal(barrier, inc=1, device_id={"tp": d}, device_id_type=pl.DeviceIdType.MESH)
    pl.semaphore_wait(barrier, 3)

    def remote(src, dst, send, recv, d):
        return pltpu.make_async_remote_copy(
            src_ref=src, dst_ref=dst, send_sem=send, recv_sem=recv,
            device_id={"tp": d}, device_id_type=pl.DeviceIdType.MESH,
        )

    def rows(i):
        return pl.ds(i * SUB, SUB)

    order_x, order_y = (0, 1, 2, 3), (2, 3, 0, 1)
    ag_x = {i: remote(x_hbm.at[rows(i)], xb.at[BX, rows(i)], ag_send.at[0, i], ag_recv.at[0, i], nx) for i in order_x}
    ag_y = {i: remote(x_hbm.at[rows(i)], xb.at[BY, rows(i)], ag_send.at[1, i], ag_recv.at[1, i], ny) for i in order_y}
    for i, j in zip(order_x, order_y):
        ag_x[i].start()
        ag_y[j].start()
    swap = [
        remote(wg_hbm, wg.at[1], w_send.at[0], w_recv.at[0], sib),
        remote(wu_hbm, wu.at[1], w_send.at[1], w_recv.at[1], sib),
        remote(wd_hbm, wd.at[pl.ds(half, half)], w_send.at[2], w_recv.at[2], sib),
    ]
    for c in swap:
        c.start()

    fw_y = [remote(xb.at[BX, rows(k)], xb.at[BD, rows(2 * k)], fw_send.at[1, k], fw_recv.at[1, k], ny) for k in range(2)]
    fw_x = [remote(xb.at[BY, rows(2 + k)], xb.at[BD, rows(2 * k + 1)], fw_send.at[0, k], fw_recv.at[0, k], nx) for k in range(2)]
    for k in range(2):
        ag_x[k].wait_recv()
        fw_y[k].start()
        ag_y[2 + k].wait_recv()
        fw_x[k].start()

    def block(x_ref, write):
        def hidden(n, _):
            s, col = n // tiles, pl.multiple_of((n % tiles) * TILE, TILE)
            gate = jnp.dot(x_ref[...], wg[s, :, pl.ds(col, TILE)], preferred_element_type=F32)
            up = jnp.dot(x_ref[...], wu[s, :, pl.ds(col, TILE)], preferred_element_type=F32)
            hid[:, pl.ds(pl.multiple_of(n * TILE, TILE), TILE)] = (jax.nn.silu(gate) * up).astype(BF16)
            return _

        def down(n, _):
            cols = pl.ds(pl.multiple_of(n * TILE, TILE), TILE)
            write(cols, jnp.dot(hid[...], wd[:, cols], preferred_element_type=F32))
            return _

        lax.fori_loop(0, 2 * tiles, hidden, None)
        lax.fori_loop(0, width // TILE, down, None)

    def into(ref, r0):
        def write(cols, v):
            ref[pl.ds(r0, UNIT), cols] = v.astype(ref.dtype)

        return write

    def unit(b, u, ref, r0):
        block(xb.at[b, pl.ds(u * UNIT, UNIT)], into(ref, r0))

    for c in local[:3]:
        c.wait()
    for c in swap:
        c.wait_recv()

    fin_x = {i: remote((px if i < 2 else sx).at[rows(i % 2)], finx.at[rows(i)], f_send.at[0, i], f_recv.at[0, i], nx) for i in range(4)}
    fin_y = {i: remote((sy if i < 2 else py).at[rows(i % 2)], finy.at[rows(i)], f_send.at[1, i], f_recv.at[1, i], ny) for i in range(4)}
    d_x = [remote(pd.at[rows(2 * k)], relx.at[rows(k)], d_send.at[0, k], d_recv.at[0, k], nx) for k in range(2)]
    d_y = [remote(pd.at[rows(2 * k + 1)], rely.at[rows(k)], d_send.at[1, k], d_recv.at[1, k], ny) for k in range(2)]

    unit(BX, 0, px, 0)
    for i in (0, 1):
        fin_x[i].start()
    unit(BY, 1, py, 0)
    for i in (2, 3):
        fin_y[i].start()
    local[3].wait()
    unit(OWN, 0, own, 0)
    for i in (2, 3):
        ag_x[i].wait_recv()
    unit(BX, 1, px32, 0)
    fw_y[0].wait_recv()
    fw_x[0].wait_recv()
    unit(BD, 0, pd, 0)
    d_x[0].start()
    d_y[0].start()
    for i in (0, 1):
        ag_y[i].wait_recv()
    unit(BY, 0, py32, 0)
    fw_y[1].wait_recv()
    fw_x[1].wait_recv()
    unit(BD, 1, pd, UNIT)
    d_x[1].start()
    d_y[1].start()
    unit(OWN, 1, own, UNIT)

    for i in (0, 1):
        fin_x[i].wait_recv()
        own[rows(i)] += finx[rows(i)].astype(F32)
    for i in (2, 3):
        fin_y[i].wait_recv()
        own[rows(i)] += finy[rows(i)].astype(F32)

    for k in range(2):
        d_x[k].wait_recv()
        sy[rows(k)] = (py32[rows(k)] + relx[rows(k)].astype(F32)).astype(BF16)
        fin_y[k].start()
        d_y[k].wait_recv()
        sx[rows(k)] = (px32[rows(k)] + rely[rows(k)].astype(F32)).astype(BF16)
        fin_x[2 + k].start()

    writes = []
    for k in range(2):
        for fin, ref, i in ((fin_x, finx, 2 + k), (fin_y, finy, k)):
            fin[i].wait_recv()
            out[rows(i)] = (own[rows(i)] + ref[rows(i)].astype(F32)).astype(BF16)
            c = pltpu.make_async_copy(out.at[rows(i)], out_hbm.at[rows(i)], out_sem.at[i])
            c.start()
            writes.append(c)

    for c in (*ag_x.values(), *ag_y.values(), *swap, *fw_x, *fw_y, *d_x, *d_y, *fin_x.values(), *fin_y.values()):
        c.wait_send()
    for c in writes:
        c.wait()


def solution(mesh):
    def step(x, w_gate, w_up, w_down):
        rows, depth = x.shape
        half, width = w_down.shape
        vmem = pltpu.VMEM
        dma = pltpu.SemaphoreType.DMA
        flops = 2 * 4 * rows * depth * 2 * half * 3
        return pl.pallas_call(
            kernel,
            out_shape=jax.ShapeDtypeStruct((rows, width), BF16),
            in_specs=[pl.BlockSpec(memory_space=pl.ANY)] * 4,
            out_specs=pl.BlockSpec(memory_space=pl.ANY),
            scratch_shapes=[
                vmem((2, depth, half), BF16),
                vmem((2, depth, half), BF16),
                vmem((2 * half, width), BF16),
                vmem((4, rows, depth), BF16),
                vmem((UNIT, 2 * half), BF16),
                vmem((rows, width), BF16),
                vmem((UNIT, width), BF16),
                vmem((UNIT, width), BF16),
                vmem((UNIT, width), F32),
                vmem((UNIT, width), F32),
                vmem((UNIT, width), BF16),
                vmem((UNIT, width), BF16),
                vmem((rows, width), F32),
                vmem((UNIT, width), BF16),
                vmem((UNIT, width), BF16),
                vmem((rows, width), BF16),
                vmem((rows, width), BF16),
                vmem((rows, width), BF16),
                dma((4,)),
                dma((4,)),
                dma((3,)),
                dma((3,)),
                dma((2, 4)),
                dma((2, 4)),
                dma((2, 2)),
                dma((2, 2)),
                dma((2, 2)),
                dma((2, 2)),
                dma((2, 4)),
                dma((2, 4)),
            ],
            compiler_params=pltpu.CompilerParams(
                collective_id=0, has_side_effects=True, vmem_limit_bytes=67_000_000
            ),
            cost_estimate=pl.CostEstimate(flops=flops, bytes_accessed=32 * 2**20, transcendentals=0),
            name="mlp",
        )(x, w_gate, w_up, w_down)

    return jax.shard_map(
        step,
        mesh=mesh,
        in_specs=(P(("dp", "tp"), None), P(None, "tp"), P(None, "tp"), P("tp", None)),
        out_specs=P(("dp", "tp"), None),
        check_vma=False,
    )
```

```python
import jax
import jax.numpy as jnp
from jax import lax
from jax.experimental import pallas as pl
from jax.experimental.pallas import tpu as pltpu
from jax.sharding import PartitionSpec as P

BF16 = jnp.bfloat16
F32 = jnp.float32

SUB = 128
UNIT = 256
TILE = 256

OWN, BX, BY, BD = 0, 1, 2, 3


def kernel(
    x_hbm, wg_hbm, wu_hbm, wd_hbm, out,
    wg, wu, wd, xb, hid, pd, px, py, px32, py32, sx, sy, own, relx, rely, finx, finy,
    loc_sem, w_send, w_recv, ag_send, ag_recv, fw_send, fw_recv, d_send, d_recv, f_send, f_recv,
):
    half = wg_hbm.shape[1]
    width = wd_hbm.shape[1]
    tiles = half // TILE

    me = lax.axis_index("tp")
    core = me % 2
    iy = (me // 2) % 2
    nx = (me + 4) % 8
    ny = me + 2 - 4 * iy
    sib = me + 1 - 2 * core

    local = [
        pltpu.make_async_copy(wg_hbm, wg.at[0], loc_sem.at[0]),
        pltpu.make_async_copy(wu_hbm, wu.at[0], loc_sem.at[1]),
        pltpu.make_async_copy(wd_hbm, wd.at[pl.ds(0, half)], loc_sem.at[2]),
        pltpu.make_async_copy(x_hbm, xb.at[OWN], loc_sem.at[3]),
    ]
    for c in local:
        c.start()

    barrier = pltpu.get_barrier_semaphore()
    for d in (nx, ny, sib):
        pl.semaphore_signal(barrier, inc=1, device_id={"tp": d}, device_id_type=pl.DeviceIdType.MESH)
    pl.semaphore_wait(barrier, 3)

    def remote(src, dst, send, recv, d):
        return pltpu.make_async_remote_copy(
            src_ref=src, dst_ref=dst, send_sem=send, recv_sem=recv,
            device_id={"tp": d}, device_id_type=pl.DeviceIdType.MESH,
        )

    def rows(i):
        return pl.ds(i * SUB, SUB)

    order_x, order_y = (0, 1, 2, 3), (2, 3, 0, 1)
    ag_x = {i: remote(x_hbm.at[rows(i)], xb.at[BX, rows(i)], ag_send.at[0, i], ag_recv.at[0, i], nx) for i in order_x}
    ag_y = {i: remote(x_hbm.at[rows(i)], xb.at[BY, rows(i)], ag_send.at[1, i], ag_recv.at[1, i], ny) for i in order_y}
    for i, j in zip(order_x, order_y):
        ag_x[i].start()
        ag_y[j].start()
    swap = [
        remote(wg_hbm, wg.at[1], w_send.at[0], w_recv.at[0], sib),
        remote(wu_hbm, wu.at[1], w_send.at[1], w_recv.at[1], sib),
        remote(wd_hbm, wd.at[pl.ds(half, half)], w_send.at[2], w_recv.at[2], sib),
    ]
    for c in swap:
        c.start()

    fw_y = [remote(xb.at[BX, rows(k)], xb.at[BD, rows(2 * k)], fw_send.at[1, k], fw_recv.at[1, k], ny) for k in range(2)]
    fw_x = [remote(xb.at[BY, rows(2 + k)], xb.at[BD, rows(2 * k + 1)], fw_send.at[0, k], fw_recv.at[0, k], nx) for k in range(2)]
    for k in range(2):
        ag_x[k].wait_recv()
        fw_y[k].start()
        ag_y[2 + k].wait_recv()
        fw_x[k].start()

    def block(x_ref, write):
        def hidden(n, _):
            s, col = n // tiles, pl.multiple_of((n % tiles) * TILE, TILE)
            gate = jnp.dot(x_ref[...], wg[s, :, pl.ds(col, TILE)], preferred_element_type=F32)
            up = jnp.dot(x_ref[...], wu[s, :, pl.ds(col, TILE)], preferred_element_type=F32)
            hid[:, pl.ds(pl.multiple_of(n * TILE, TILE), TILE)] = (jax.nn.silu(gate) * up).astype(BF16)
            return _

        def down(n, _):
            cols = pl.ds(pl.multiple_of(n * TILE, TILE), TILE)
            write(cols, jnp.dot(hid[...], wd[:, cols], preferred_element_type=F32))
            return _

        lax.fori_loop(0, 2 * tiles, hidden, None)
        lax.fori_loop(0, width // TILE, down, None)

    def into(ref, r0):
        def write(cols, v):
            ref[pl.ds(r0, UNIT), cols] = v.astype(ref.dtype)

        return write

    def unit(b, u, ref, r0):
        block(xb.at[b, pl.ds(u * UNIT, UNIT)], into(ref, r0))

    for c in local[:3]:
        c.wait()
    for c in swap:
        c.wait_recv()

    fin_x = {i: remote((px if i < 2 else sx).at[rows(i % 2)], finx.at[rows(i)], f_send.at[0, i], f_recv.at[0, i], nx) for i in range(4)}
    fin_y = {i: remote((sy if i < 2 else py).at[rows(i % 2)], finy.at[rows(i)], f_send.at[1, i], f_recv.at[1, i], ny) for i in range(4)}
    d_x = [remote(pd.at[rows(2 * k)], relx.at[rows(k)], d_send.at[0, k], d_recv.at[0, k], nx) for k in range(2)]
    d_y = [remote(pd.at[rows(2 * k + 1)], rely.at[rows(k)], d_send.at[1, k], d_recv.at[1, k], ny) for k in range(2)]

    unit(BX, 0, px, 0)
    for i in (0, 1):
        fin_x[i].start()
    unit(BY, 1, py, 0)
    for i in (2, 3):
        fin_y[i].start()
    local[3].wait()
    unit(OWN, 0, own, 0)
    for i in (2, 3):
        ag_x[i].wait_recv()
    unit(BX, 1, px32, 0)
    fw_y[0].wait_recv()
    fw_x[0].wait_recv()
    unit(BD, 0, pd, 0)
    d_x[0].start()
    d_y[0].start()
    for i in (0, 1):
        ag_y[i].wait_recv()
    unit(BY, 0, py32, 0)
    fw_y[1].wait_recv()
    fw_x[1].wait_recv()
    unit(BD, 1, pd, UNIT)
    d_x[1].start()
    d_y[1].start()
    unit(OWN, 1, own, UNIT)

    for i in (0, 1):
        fin_x[i].wait_recv()
        own[rows(i)] += finx[rows(i)].astype(F32)
    for i in (2, 3):
        fin_y[i].wait_recv()
        own[rows(i)] += finy[rows(i)].astype(F32)

    for k in range(2):
        d_x[k].wait_recv()
        sy[rows(k)] = (py32[rows(k)] + relx[rows(k)].astype(F32)).astype(BF16)
        fin_y[k].start()
        d_y[k].wait_recv()
        sx[rows(k)] = (px32[rows(k)] + rely[rows(k)].astype(F32)).astype(BF16)
        fin_x[2 + k].start()

    for k in range(2):
        for fin, ref, i in ((fin_x, finx, 2 + k), (fin_y, finy, k)):
            fin[i].wait_recv()
            out[rows(i)] = (own[rows(i)] + ref[rows(i)].astype(F32)).astype(BF16)

    for c in (*ag_x.values(), *ag_y.values(), *swap, *fw_x, *fw_y, *d_x, *d_y, *fin_x.values(), *fin_y.values()):
        c.wait_send()


def solution(mesh):
    def step(x, w_gate, w_up, w_down):
        rows, depth = x.shape
        half, width = w_down.shape
        vmem = pltpu.VMEM
        dma = pltpu.SemaphoreType.DMA
        flops = 2 * 4 * rows * depth * 2 * half * 3
        return pl.pallas_call(
            kernel,
            out_shape=pltpu.VMEM((rows, width), BF16),
            in_specs=[pl.BlockSpec(memory_space=pl.ANY)] * 4,
            out_specs=pl.BlockSpec(memory_space=pltpu.VMEM),
            scratch_shapes=[
                vmem((2, depth, half), BF16),
                vmem((2, depth, half), BF16),
                vmem((2 * half, width), BF16),
                vmem((4, rows, depth), BF16),
                vmem((UNIT, 2 * half), BF16),
                vmem((rows, width), BF16),
                vmem((UNIT, width), BF16),
                vmem((UNIT, width), BF16),
                vmem((UNIT, width), F32),
                vmem((UNIT, width), F32),
                vmem((UNIT, width), BF16),
                vmem((UNIT, width), BF16),
                vmem((rows, width), F32),
                vmem((UNIT, width), BF16),
                vmem((UNIT, width), BF16),
                vmem((rows, width), BF16),
                vmem((rows, width), BF16),
                dma((4,)),
                dma((3,)),
                dma((3,)),
                dma((2, 4)),
                dma((2, 4)),
                dma((2, 2)),
                dma((2, 2)),
                dma((2, 2)),
                dma((2, 2)),
                dma((2, 4)),
                dma((2, 4)),
            ],
            compiler_params=pltpu.CompilerParams(
                collective_id=0, has_side_effects=True, vmem_limit_bytes=60 * 2**20
            ),
            cost_estimate=pl.CostEstimate(flops=flops, bytes_accessed=32 * 2**20, transcendentals=0),
            name="mlp",
        )(x, w_gate, w_up, w_down)

    return jax.shard_map(
        step,
        mesh=mesh,
        in_specs=(P(("dp", "tp"), None), P(None, "tp"), P(None, "tp"), P("tp", None)),
        out_specs=P(("dp", "tp"), None),
        check_vma=False,
    )
```

```python
import jax
import jax.numpy as jnp
from jax import lax
from jax.experimental import pallas as pl
from jax.experimental.pallas import tpu as pltpu
from jax.sharding import PartitionSpec as P

BF16 = jnp.bfloat16
F32 = jnp.float32
MESH = pl.DeviceIdType.MESH

SUB = 128
UNIT = 256
TILE = 256

OWN, BX, BY, BD = 0, 1, 2, 3

RELAY = ((0, 128, 0), (128, 96, 1), (224, 32, 1))


def kernel(
    x_hbm, wg_hbm, wu_hbm, wd_hbm, out,
    w, wd, xb, hid, pd, px, py, px32, py32, sx, sy, own, relx, rely, finx, finy,
    ready, w_sem, x_sem, swap_send, swap_recv, send, ag_recv, fw_recv, d_recv, plain_recv, f_recv,
):
    half = wg_hbm.shape[1]
    width = wd_hbm.shape[1]
    tiles = half // TILE

    me = lax.axis_index("tp")
    core = me % 2
    iy = (me // 2) % 2
    ix = me // 4
    nx = (me + 4) % 8
    ny = me + 2 - 4 * iy
    sib = me + 1 - 2 * core

    barrier = pltpu.get_barrier_semaphore()
    pairs = ((ix, nx, 0), (iy, ny, 1), (1 - core, sib, 2))

    for late, d, _ in pairs:
        @pl.when(late == 0)
        def _():
            pl.semaphore_signal(barrier, inc=1, device_id={"tp": d}, device_id_type=MESH)

    local = [
        pltpu.make_async_copy(wg_hbm, w.at[0], w_sem),
        pltpu.make_async_copy(wu_hbm, w.at[2], w_sem),
        pltpu.make_async_copy(wd_hbm, wd.at[pl.ds(0, half)], w_sem),
    ]
    for c in local:
        c.start()
    own_x = pltpu.make_async_copy(x_hbm, xb.at[OWN], x_sem)
    own_x.start()

    first = ix + iy + 1 - core

    @pl.when(first > 0)
    def _():
        pl.semaphore_wait(barrier, first)

    for late, d, i in pairs:
        @pl.when(late == 1)
        def _():
            pl.semaphore_signal(ready.at[i], inc=1, device_id={"tp": d}, device_id_type=MESH)

    def remote(src, dst, recv, d, sem=send):
        return pltpu.make_async_remote_copy(
            src_ref=src, dst_ref=dst, send_sem=sem, recv_sem=recv, device_id={"tp": d}, device_id_type=MESH
        )

    def rows(i):
        return pl.ds(i * SUB, SUB)

    group = (0, 1, 2, 2)
    ag_x = [remote(x_hbm.at[rows(i)], xb.at[BX, rows(i)], ag_recv.at[g], nx) for i, g in zip((0, 1, 2, 3), group)]
    ag_y = [remote(x_hbm.at[rows(i)], xb.at[BY, rows(i)], ag_recv.at[g], ny) for i, g in zip((2, 3, 0, 1), group)]
    swap = [
        remote(wg_hbm, w.at[1], swap_recv, sib, swap_send),
        remote(wu_hbm, w.at[3], swap_recv, sib, swap_send),
        remote(wd_hbm, wd.at[pl.ds(half, half)], swap_recv, sib, swap_send),
    ]
    copies = (ag_x, ag_y, swap)
    for now in (1, 0):
        for late, _, i in pairs:
            @pl.when(late == now)
            def _():
                if not now:
                    pl.semaphore_wait(ready.at[i], 1)
                for c in copies[i]:
                    c.start()

    def wait(ref, sem):
        pltpu.make_async_copy(ref, ref, sem).wait()

    fw_y = [remote(xb.at[BX, rows(k)], xb.at[BD, rows(2 * k)], fw_recv.at[k], ny) for k in range(2)]
    fw_x = [remote(xb.at[BY, rows(2 + k)], xb.at[BD, rows(2 * k + 1)], fw_recv.at[k], nx) for k in range(2)]
    pair = pl.ds(0, 2 * SUB)
    for k in range(2):
        wait(xb.at[BX, pair], ag_recv.at[k])
        fw_y[k].start()
        fw_x[k].start()

    def unit(b, u, ref, r0):
        x_ref = xb.at[b, pl.ds(u * UNIT, UNIT)]

        def hidden(n, _):
            s, col = n // tiles, pl.ds(pl.multiple_of((n % tiles) * TILE, TILE), TILE)
            gate = jnp.dot(x_ref[...], w[s, :, col], preferred_element_type=F32)
            up = jnp.dot(x_ref[...], w[2 + s, :, col], preferred_element_type=F32)
            hid[:, pl.ds(pl.multiple_of(n * TILE, TILE), TILE)] = (jax.nn.silu(gate) * up).astype(BF16)
            return _

        def down(n, _):
            cols = pl.ds(pl.multiple_of(n * TILE, TILE), TILE)
            v = jnp.dot(hid[...], wd[:, cols], preferred_element_type=F32)
            ref[pl.ds(r0, UNIT), cols] = v.astype(ref.dtype)
            return _

        lax.fori_loop(0, 2 * tiles, hidden, None)
        lax.fori_loop(0, width // TILE, down, None)

    weights = pl.ds(0, 3)
    wait(w.at[weights], w_sem)
    wait(w.at[weights], swap_recv)

    d_x = [remote(pd.at[rows(2 * k)], relx.at[rows(k)], d_recv.at[k], nx) for k in range(2)]
    d_y = [remote(pd.at[rows(2 * k + 1)], rely.at[rows(k)], d_recv.at[k], ny) for k in range(2)]
    low, high = pl.ds(0, UNIT), pl.ds(UNIT, UNIT)

    unit(BX, 0, px, 0)
    remote(px, finx.at[low], plain_recv, nx).start()
    unit(BY, 1, py, 0)
    remote(py, finy.at[high], plain_recv, ny).start()
    own_x.wait()
    unit(OWN, 0, own, 0)
    wait(xb.at[BX], ag_recv.at[2])
    unit(BX, 1, px32, 0)
    wait(xb.at[BD, pair], fw_recv.at[0])
    unit(BD, 0, pd, 0)
    d_x[0].start()
    d_y[0].start()
    unit(BY, 0, py32, 0)
    wait(xb.at[BD, pair], fw_recv.at[1])
    unit(BD, 1, pd, UNIT)
    d_x[1].start()
    d_y[1].start()
    unit(OWN, 1, own, UNIT)

    wait(finx, plain_recv)
    own[low] += finx[low].astype(F32)
    own[high] += finy[high].astype(F32)

    for i, (r0, n, k) in enumerate(RELAY):
        if i == 0 or k != RELAY[i - 1][2]:
            wait(relx.at[pair], d_recv.at[k])
        r = pl.ds(r0, n)
        sy[r] = (py32[r] + relx[r].astype(F32)).astype(BF16)
        remote(sy.at[r], finy.at[r], f_recv.at[i], ny).start()
        sx[r] = (px32[r] + rely[r].astype(F32)).astype(BF16)
        remote(sx.at[r], finx.at[pl.ds(UNIT + r0, n)], f_recv.at[i], nx).start()

    wait(w.at[weights], swap_send)
    for i, (r0, n, _) in enumerate(RELAY):
        wait(finx.at[pl.ds(0, 2 * n)], f_recv.at[i])
        a, b = pl.ds(r0, n), pl.ds(UNIT + r0, n)
        out[a] = (own[a] + finy[a].astype(F32)).astype(BF16)
        out[b] = (own[b] + finx[b].astype(F32)).astype(BF16)
    wait(w.at[weights], send)


def solution(mesh):
    def step(x, w_gate, w_up, w_down):
        rows, depth = x.shape
        half, width = w_down.shape
        vmem = pltpu.VMEM
        dma = pltpu.SemaphoreType.DMA
        flops = 2 * 4 * rows * depth * 2 * half * 3
        return pl.pallas_call(
            kernel,
            out_shape=pltpu.VMEM((rows, width), BF16),
            in_specs=[pl.BlockSpec(memory_space=pl.ANY)] * 4,
            out_specs=pl.BlockSpec(memory_space=pltpu.VMEM),
            scratch_shapes=[
                vmem((4, depth, half), BF16),
                vmem((2 * half, width), BF16),
                vmem((4, rows, depth), BF16),
                vmem((UNIT, 2 * half), BF16),
                vmem((rows, width), BF16),
                vmem((UNIT, width), BF16),
                vmem((UNIT, width), BF16),
                vmem((UNIT, width), F32),
                vmem((UNIT, width), F32),
                vmem((UNIT, width), BF16),
                vmem((UNIT, width), BF16),
                vmem((rows, width), F32),
                vmem((UNIT, width), BF16),
                vmem((UNIT, width), BF16),
                vmem((rows, width), BF16),
                vmem((rows, width), BF16),
                pltpu.SemaphoreType.REGULAR((3,)),
                dma,
                dma,
                dma,
                dma,
                dma,
                dma((3,)),
                dma((2,)),
                dma((2,)),
                dma,
                dma((len(RELAY),)),
            ],
            compiler_params=pltpu.CompilerParams(
                collective_id=0, has_side_effects=True, vmem_limit_bytes=60 * 2**20
            ),
            cost_estimate=pl.CostEstimate(flops=flops, bytes_accessed=32 * 2**20, transcendentals=0),
            name="mlp",
        )(x, w_gate, w_up, w_down)

    return jax.shard_map(
        step,
        mesh=mesh,
        in_specs=(P(("dp", "tp"), None), P(None, "tp"), P(None, "tp"), P("tp", None)),
        out_specs=P(("dp", "tp"), None),
        check_vma=False,
    )
```

```python
import jax
import jax.numpy as jnp
from jax import lax
from jax.experimental import pallas as pl
from jax.experimental.pallas import tpu as pltpu
from jax.sharding import PartitionSpec as P

BF16 = jnp.bfloat16
F32 = jnp.float32
MESH = pl.DeviceIdType.MESH

SUB = 128
UNIT = 256
TILE = 256

OWN, BX, BY, BD = 0, 1, 2, 3

RELAY = ((0, 32, 0), (32, 96, 0), (128, 96, 1), (224, 32, 1))


def kernel(
    x_hbm, wg_hbm, wu_hbm, wd_hbm, out,
    w, wd, xb, hid, pd, px, py, px32, py32, sx, sy, own, relx, rely, finx, finy,
    ready, turn, w_sem, x_sem, swap_send, swap_recv, send, lead_send, ag_recv, fw_recv, d_recv, plain_recv, f_recv,
):
    half = wg_hbm.shape[1]
    width = wd_hbm.shape[1]
    tiles = half // TILE

    me = lax.axis_index("tp")
    core = me % 2
    iy = (me // 2) % 2
    ix = me // 4
    nx = (me + 4) % 8
    ny = me + 2 - 4 * iy
    sib = me + 1 - 2 * core

    barrier = pltpu.get_barrier_semaphore()
    pairs = ((ix, nx, 0), (iy, ny, 1), (1 - core, sib, 2))

    for late, d, _ in pairs:
        @pl.when(late == 0)
        def _():
            pl.semaphore_signal(barrier, inc=1, device_id={"tp": d}, device_id_type=MESH)

    local = [
        pltpu.make_async_copy(wg_hbm, w.at[0], w_sem),
        pltpu.make_async_copy(wu_hbm, w.at[2], w_sem),
        pltpu.make_async_copy(wd_hbm, wd.at[pl.ds(0, half)], w_sem),
    ]
    for c in local:
        c.start()
    own_x = pltpu.make_async_copy(x_hbm, xb.at[OWN], x_sem)
    own_x.start()

    first = ix + iy + 1 - core

    @pl.when(first > 0)
    def _():
        pl.semaphore_wait(barrier, first)

    for late, d, i in pairs:
        @pl.when(late == 1)
        def _():
            pl.semaphore_signal(ready.at[i], inc=1, device_id={"tp": d}, device_id_type=MESH)

    def remote(src, dst, recv, d, sem=send):
        return pltpu.make_async_remote_copy(
            src_ref=src, dst_ref=dst, send_sem=sem, recv_sem=recv, device_id={"tp": d}, device_id_type=MESH
        )

    def rows(i):
        return pl.ds(i * SUB, SUB)

    group = (0, 1, 2, 2)
    ag_x = [remote(x_hbm.at[rows(i)], xb.at[BX, rows(i)], ag_recv.at[g], nx) for i, g in zip((0, 1, 2, 3), group)]
    ag_y = [remote(x_hbm.at[rows(i)], xb.at[BY, rows(i)], ag_recv.at[g], ny) for i, g in zip((2, 3, 0, 1), group)]
    swap = [
        remote(wg_hbm, w.at[1], swap_recv, sib, swap_send),
        remote(wu_hbm, w.at[3], swap_recv, sib, swap_send),
        remote(wd_hbm, wd.at[pl.ds(half, half)], swap_recv, sib, swap_send),
    ]
    copies = (ag_x, ag_y, swap)
    for now in (1, 0):
        for late, _, i in pairs:
            @pl.when(late == now)
            def _():
                if not now:
                    pl.semaphore_wait(ready.at[i], 1)
                for c in copies[i]:
                    c.start()

    def wait(ref, sem):
        pltpu.make_async_copy(ref, ref, sem).wait()

    fw_y = [remote(xb.at[BX, rows(k)], xb.at[BD, rows(2 * k)], fw_recv.at[k], ny) for k in range(2)]
    fw_x = [remote(xb.at[BY, rows(2 + k)], xb.at[BD, rows(2 * k + 1)], fw_recv.at[k], nx) for k in range(2)]
    pair = pl.ds(0, 2 * SUB)
    for k in range(2):
        wait(xb.at[BX, pair], ag_recv.at[k])
        fw_y[k].start()
        fw_x[k].start()

    def unit(b, u, ref, r0):
        x_ref = xb.at[b, pl.ds(u * UNIT, UNIT)]

        def hidden(n, _):
            s, col = n // tiles, pl.ds(pl.multiple_of((n % tiles) * TILE, TILE), TILE)
            gate = jnp.dot(x_ref[...], w[s, :, col], preferred_element_type=F32)
            up = jnp.dot(x_ref[...], w[2 + s, :, col], preferred_element_type=F32)
            hid[:, pl.ds(pl.multiple_of(n * TILE, TILE), TILE)] = (jax.nn.silu(gate) * up).astype(BF16)
            return _

        def down(n, _):
            cols = pl.ds(pl.multiple_of(n * TILE, TILE), TILE)
            v = jnp.dot(hid[...], wd[:, cols], preferred_element_type=F32)
            ref[pl.ds(r0, UNIT), cols] = v.astype(ref.dtype)
            return _

        lax.fori_loop(0, 2 * tiles, hidden, None)
        lax.fori_loop(0, width // TILE, down, None)

    weights = pl.ds(0, 3)
    wait(w.at[weights], w_sem)
    wait(w.at[weights], swap_recv)

    d_x = [remote(pd.at[rows(2 * k)], relx.at[rows(k)], d_recv.at[k], nx) for k in range(2)]
    d_y = [remote(pd.at[rows(2 * k + 1)], rely.at[rows(k)], d_recv.at[k], ny) for k in range(2)]
    low, high = pl.ds(0, UNIT), pl.ds(UNIT, UNIT)

    unit(BX, 0, px, 0)
    remote(px, finx.at[low], plain_recv, nx).start()
    unit(BY, 1, py, 0)
    remote(py, finy.at[high], plain_recv, ny).start()
    own_x.wait()
    unit(OWN, 0, own, 0)
    wait(xb.at[BX], ag_recv.at[2])
    unit(BX, 1, px32, 0)
    wait(xb.at[BD, pair], fw_recv.at[0])
    unit(BD, 0, pd, 0)
    d_x[0].start()
    d_y[0].start()
    unit(BY, 0, py32, 0)
    wait(xb.at[BD, pair], fw_recv.at[1])
    unit(BD, 1, pd, UNIT)
    d_x[1].start()
    d_y[1].start()
    unit(OWN, 1, own, UNIT)

    wait(finx, plain_recv)
    own[low] += finx[low].astype(F32)
    own[high] += finy[high].astype(F32)

    def relay(i):
        r0, n, _ = RELAY[i]
        r = pl.ds(r0, n)
        sy[r] = (py32[r] + relx[r].astype(F32)).astype(BF16)
        sx[r] = (px32[r] + rely[r].astype(F32)).astype(BF16)
        sems = (lead_send.at[0], lead_send.at[1]) if i == 0 else (send, send)
        return (
            remote(sx.at[r], finx.at[pl.ds(UNIT + r0, n)], f_recv.at[i], nx, sems[0]),
            remote(sy.at[r], finy.at[r], f_recv.at[i], ny, sems[1]),
        )

    lead = pl.ds(0, RELAY[0][1])
    wait(relx.at[pair], d_recv.at[0])
    head, rest = relay(0), relay(1)

    def go(i):
        @pl.when(core == 1)
        def _():
            pl.semaphore_wait(turn.at[i], 1)

        head[i].start()
        rest[i].start()

    def done(i):
        @pl.when(core == 0)
        def _():
            wait(finx.at[lead], lead_send.at[i])
            pl.semaphore_signal(turn.at[i], inc=1, device_id={"tp": sib}, device_id_type=MESH)

    for early, order in ((1, (0, 1)), (0, (1, 0))):
        @pl.when(ix == early)
        def _():
            for i in order:
                go(i)
            for i in order:
                done(i)

    wait(relx.at[pair], d_recv.at[1])
    for i in (2, 3):
        for c in relay(i):
            c.start()

    wait(w.at[weights], swap_send)
    for i, (r0, n, _) in enumerate(RELAY):
        wait(finx.at[pl.ds(0, 2 * n)], f_recv.at[i])
        a, b = pl.ds(r0, n), pl.ds(UNIT + r0, n)
        out[a] = (own[a] + finy[a].astype(F32)).astype(BF16)
        out[b] = (own[b] + finx[b].astype(F32)).astype(BF16)

    @pl.when(core == 1)
    def _():
        for i in (0, 1):
            wait(finx.at[lead], lead_send.at[i])

    wait(w.at[:, pl.ds(0, 3 * half // 2 - RELAY[0][1])], send)


def solution(mesh):
    def step(x, w_gate, w_up, w_down):
        rows, depth = x.shape
        half, width = w_down.shape
        vmem = pltpu.VMEM
        dma = pltpu.SemaphoreType.DMA
        flops = 2 * 4 * rows * depth * 2 * half * 3
        return pl.pallas_call(
            kernel,
            out_shape=pltpu.VMEM((rows, width), BF16),
            in_specs=[pl.BlockSpec(memory_space=pl.ANY)] * 4,
            out_specs=pl.BlockSpec(memory_space=pltpu.VMEM),
            scratch_shapes=[
                vmem((4, depth, half), BF16),
                vmem((2 * half, width), BF16),
                vmem((4, rows, depth), BF16),
                vmem((UNIT, 2 * half), BF16),
                vmem((rows, width), BF16),
                vmem((UNIT, width), BF16),
                vmem((UNIT, width), BF16),
                vmem((UNIT, width), F32),
                vmem((UNIT, width), F32),
                vmem((UNIT, width), BF16),
                vmem((UNIT, width), BF16),
                vmem((rows, width), F32),
                vmem((UNIT, width), BF16),
                vmem((UNIT, width), BF16),
                vmem((rows, width), BF16),
                vmem((rows, width), BF16),
                pltpu.SemaphoreType.REGULAR((3,)),
                pltpu.SemaphoreType.REGULAR((2,)),
                dma,
                dma,
                dma,
                dma,
                dma,
                dma((2,)),
                dma((3,)),
                dma((2,)),
                dma((2,)),
                dma,
                dma((len(RELAY),)),
            ],
            compiler_params=pltpu.CompilerParams(
                collective_id=0, has_side_effects=True, vmem_limit_bytes=60 * 2**20
            ),
            cost_estimate=pl.CostEstimate(flops=flops, bytes_accessed=32 * 2**20, transcendentals=0),
            name="mlp",
        )(x, w_gate, w_up, w_down)

    return jax.shard_map(
        step,
        mesh=mesh,
        in_specs=(P(("dp", "tp"), None), P(None, "tp"), P(None, "tp"), P("tp", None)),
        out_specs=P(("dp", "tp"), None),
        check_vma=False,
    )
```

```python
import jax
import jax.numpy as jnp
from jax import lax
from jax.experimental import pallas as pl
from jax.experimental.pallas import tpu as pltpu
from jax.sharding import PartitionSpec as P

BF16 = jnp.bfloat16
F32 = jnp.float32
MESH = pl.DeviceIdType.MESH

SUB = 128
UNIT = 256
TILE = 256

OWN, BX, BY, BD = 0, 1, 2, 3

RELAY = ((0, 32, 0), (32, 96, 0), (128, 112, 1), (240, 16, 1))


def kernel(
    x_hbm, wg_hbm, wu_hbm, wd_hbm, out,
    w, wd, xb, hid, pd, px, py, px32, py32, sx, sy, own, relx, rely, finx, finy,
    ready, turn, w_sem, swap_send, swap_recv, send, lead_send, ag_recv, fw_recv, d_recv, plain_recv, f_recv,
):
    half = wg_hbm.shape[1]
    width = wd_hbm.shape[1]
    tiles = half // TILE

    me = lax.axis_index("tp")
    core = me % 2
    iy = (me // 2) % 2
    ix = me // 4
    nx = (me + 4) % 8
    ny = me + 2 - 4 * iy
    sib = me + 1 - 2 * core

    barrier = pltpu.get_barrier_semaphore()
    pairs = ((ix, nx, 0), (iy, ny, 1), (1 - core, sib, 2))

    for late, d, _ in pairs:
        @pl.when(late == 0)
        def _():
            pl.semaphore_signal(barrier, inc=1, device_id={"tp": d}, device_id_type=MESH)

    first = ix + iy + 1 - core

    @pl.when(first > 0)
    def _():
        pl.semaphore_wait(barrier, first)

    for late, d, _ in pairs:
        @pl.when(late == 1)
        def _():
            pl.semaphore_signal(ready, inc=1, device_id={"tp": d}, device_id_type=MESH)

    def remote(src, dst, recv, d, sem=send):
        return pltpu.make_async_remote_copy(
            src_ref=src, dst_ref=dst, send_sem=sem, recv_sem=recv, device_id={"tp": d}, device_id_type=MESH
        )

    def rows(i):
        return pl.ds(i * SUB, SUB)

    group = (0, 1, 2, 2)
    ag_x = [remote(x_hbm.at[rows(i)], xb.at[BX, rows(i)], ag_recv.at[g], nx) for i, g in zip((0, 1, 2, 3), group)]
    ag_y = [remote(x_hbm.at[rows(i)], xb.at[BY, rows(i)], ag_recv.at[g], ny) for i, g in zip((2, 3, 0, 1), group)]
    swap = [
        remote(wg_hbm, w.at[1], swap_recv, sib, swap_send),
        remote(wu_hbm, w.at[3], swap_recv, sib, swap_send),
        remote(wd_hbm, wd.at[pl.ds(half, half)], swap_recv, sib, swap_send),
    ]
    copies = (ag_x, ag_y, swap)

    def start(now):
        for late, _, i in pairs:
            @pl.when(late == now)
            def _():
                for c in copies[i]:
                    c.start()

    start(1)
    local = [
        pltpu.make_async_copy(wg_hbm, w.at[0], w_sem),
        pltpu.make_async_copy(wu_hbm, w.at[2], w_sem),
        pltpu.make_async_copy(wd_hbm, wd.at[pl.ds(0, half)], w_sem),
        pltpu.make_async_copy(x_hbm, xb.at[OWN], w_sem),
    ]
    for c in local:
        c.start()

    @pl.when(first < 3)
    def _():
        pl.semaphore_wait(ready, 3 - first)

    start(0)

    def wait(ref, sem):
        pltpu.make_async_copy(ref, ref, sem).wait()

    fw_y = [remote(xb.at[BX, rows(k)], xb.at[BD, rows(2 * k)], fw_recv.at[k], ny) for k in range(2)]
    fw_x = [remote(xb.at[BY, rows(2 + k)], xb.at[BD, rows(2 * k + 1)], fw_recv.at[k], nx) for k in range(2)]
    pair = pl.ds(0, 2 * SUB)
    for k in range(2):
        wait(xb.at[BX, pair], ag_recv.at[k])
        fw_y[k].start()
        fw_x[k].start()

    def unit(b, u, ref, r0):
        x_ref = xb.at[b, pl.ds(u * UNIT, UNIT)]

        def hidden(n, _):
            s, col = n // tiles, pl.ds(pl.multiple_of((n % tiles) * TILE, TILE), TILE)
            gate = jnp.dot(x_ref[...], w[s, :, col], preferred_element_type=F32)
            up = jnp.dot(x_ref[...], w[2 + s, :, col], preferred_element_type=F32)
            hid[:, pl.ds(pl.multiple_of(n * TILE, TILE), TILE)] = (jax.nn.silu(gate) * up).astype(BF16)
            return _

        def down(n, _):
            cols = pl.ds(pl.multiple_of(n * TILE, TILE), TILE)
            v = jnp.dot(hid[...], wd[:, cols], preferred_element_type=F32)
            ref[pl.ds(r0, UNIT), cols] = v.astype(ref.dtype)
            return _

        lax.fori_loop(0, 2 * tiles, hidden, None)
        lax.fori_loop(0, width // TILE, down, None)

    weights = pl.ds(0, 3)
    wait(w.at[:, pl.ds(0, 7 * half // 4)], w_sem)
    wait(w.at[weights], swap_recv)

    d_x = [remote(pd.at[rows(2 * k)], relx.at[rows(k)], d_recv.at[k], nx) for k in range(2)]
    d_y = [remote(pd.at[rows(2 * k + 1)], rely.at[rows(k)], d_recv.at[k], ny) for k in range(2)]
    low, high = pl.ds(0, UNIT), pl.ds(UNIT, UNIT)

    unit(BX, 0, px, 0)
    remote(px, finx.at[low], plain_recv, nx).start()
    unit(BY, 1, py, 0)
    remote(py, finy.at[high], plain_recv, ny).start()
    unit(OWN, 0, own, 0)
    wait(xb.at[BX], ag_recv.at[2])
    unit(BX, 1, px32, 0)
    wait(xb.at[BD, pair], fw_recv.at[0])
    unit(BD, 0, pd, 0)
    d_x[0].start()
    d_y[0].start()
    unit(BY, 0, py32, 0)
    wait(xb.at[BD, pair], fw_recv.at[1])
    unit(BD, 1, pd, UNIT)
    d_x[1].start()
    d_y[1].start()
    unit(OWN, 1, own, UNIT)

    wait(finx, plain_recv)
    own[low] += finx[low].astype(F32)
    own[high] += finy[high].astype(F32)

    def relay(i):
        r0, n, _ = RELAY[i]
        r = pl.ds(r0, n)
        sy[r] = (py32[r] + relx[r].astype(F32)).astype(BF16)
        sx[r] = (px32[r] + rely[r].astype(F32)).astype(BF16)
        sem = lead_send if i == 0 else send
        return (
            remote(sx.at[r], finx.at[pl.ds(UNIT + r0, n)], f_recv.at[i], nx, sem),
            remote(sy.at[r], finy.at[r], f_recv.at[i], ny, sem),
        )

    lead = pl.ds(0, 2 * RELAY[0][1])
    wait(relx.at[pair], d_recv.at[0])
    head, rest = relay(0), relay(1)

    @pl.when(core == 1)
    def _():
        pl.semaphore_wait(turn, 1)

    for c in (*head, *rest):
        c.start()
    wait(finx.at[lead], lead_send)

    @pl.when(core == 0)
    def _():
        pl.semaphore_signal(turn, inc=1, device_id={"tp": sib}, device_id_type=MESH)

    wait(relx.at[pair], d_recv.at[1])
    for i in (2, 3):
        for c in relay(i):
            c.start()

    wait(w.at[weights], swap_send)
    for i, (r0, n, _) in enumerate(RELAY):
        wait(finx.at[pl.ds(0, 2 * n)], f_recv.at[i])
        a, b = pl.ds(r0, n), pl.ds(UNIT + r0, n)
        out[a] = (own[a] + finy[a].astype(F32)).astype(BF16)
        out[b] = (own[b] + finx[b].astype(F32)).astype(BF16)

    wait(w.at[:, pl.ds(0, 3 * half // 2 - RELAY[0][1])], send)


def solution(mesh):
    def step(x, w_gate, w_up, w_down):
        rows, depth = x.shape
        half, width = w_down.shape
        vmem = pltpu.VMEM
        dma = pltpu.SemaphoreType.DMA
        flops = 2 * 4 * rows * depth * 2 * half * 3
        return pl.pallas_call(
            kernel,
            out_shape=pltpu.VMEM((rows, width), BF16),
            in_specs=[pl.BlockSpec(memory_space=pl.ANY)] * 4,
            out_specs=pl.BlockSpec(memory_space=pltpu.VMEM),
            scratch_shapes=[
                vmem((4, depth, half), BF16),
                vmem((2 * half, width), BF16),
                vmem((4, rows, depth), BF16),
                vmem((UNIT, 2 * half), BF16),
                vmem((rows, width), BF16),
                vmem((UNIT, width), BF16),
                vmem((UNIT, width), BF16),
                vmem((UNIT, width), F32),
                vmem((UNIT, width), F32),
                vmem((UNIT, width), BF16),
                vmem((UNIT, width), BF16),
                vmem((rows, width), F32),
                vmem((UNIT, width), BF16),
                vmem((UNIT, width), BF16),
                vmem((rows, width), BF16),
                vmem((rows, width), BF16),
                pltpu.SemaphoreType.REGULAR,
                pltpu.SemaphoreType.REGULAR,
                dma,
                dma,
                dma,
                dma,
                dma,
                dma((3,)),
                dma((2,)),
                dma((2,)),
                dma,
                dma((len(RELAY),)),
            ],
            compiler_params=pltpu.CompilerParams(
                collective_id=0, has_side_effects=True, vmem_limit_bytes=60 * 2**20
            ),
            cost_estimate=pl.CostEstimate(flops=flops, bytes_accessed=32 * 2**20, transcendentals=0),
            name="mlp",
        )(x, w_gate, w_up, w_down)

    return jax.shard_map(
        step,
        mesh=mesh,
        in_specs=(P(("dp", "tp"), None), P(None, "tp"), P(None, "tp"), P("tp", None)),
        out_specs=P(("dp", "tp"), None),
        check_vma=False,
    )
```

```python
import jax
import jax.numpy as jnp
from jax import lax
from jax.experimental import pallas as pl
from jax.experimental.pallas import tpu as pltpu
from jax.sharding import PartitionSpec as P

BF16 = jnp.bfloat16
F32 = jnp.float32
MESH = pl.DeviceIdType.MESH

SUB = 128
UNIT = 256
TILE = 256

OWN, BX, BY, BD = 0, 1, 2, 3

RELAY = ((0, 32, 0), (32, 96, 0), (128, 112, 1), (240, 16, 1))
TAIL = RELAY[-1][1]


def kernel(
    x_hbm, wg_hbm, wu_hbm, wd_hbm, out, tail_own, tail_fin,
    w, wd, xb, hid, pd, px, py, px32, py32, sx, sy, own, relx, rely, finx, finy,
    ready, turn, sems,
):
    ag_recv = (sems.at[0], sems.at[1], sems.at[2])
    fw_recv = (sems.at[2], sems.at[3])
    d_recv = (sems.at[4], sems.at[5])
    f_recv = (sems.at[6], sems.at[6], sems.at[6], sems.at[7])
    send, lead_send = sems.at[8], sems.at[9]
    w_sem, swap_recv, swap_send, plain_recv = ag_recv[0], ag_recv[1], lead_send, d_recv[0]

    half = wg_hbm.shape[1]
    width = wd_hbm.shape[1]
    tiles = half // TILE

    me = lax.axis_index("tp")
    core = me % 2
    iy = (me // 2) % 2
    ix = me // 4
    nx = (me + 4) % 8
    ny = me + 2 - 4 * iy
    sib = me + 1 - 2 * core

    barrier = pltpu.get_barrier_semaphore()
    pairs = ((ix, nx, 0), (iy, ny, 1), (1 - core, sib, 2))

    for late, d, _ in pairs:
        @pl.when(late == 0)
        def _():
            pl.semaphore_signal(barrier, inc=1, device_id={"tp": d}, device_id_type=MESH)

    first = ix + iy + 1 - core

    @pl.when(first > 0)
    def _():
        pl.semaphore_wait(barrier, first)

    for late, d, _ in pairs:
        @pl.when(late == 1)
        def _():
            pl.semaphore_signal(ready, inc=1, device_id={"tp": d}, device_id_type=MESH)

    def remote(src, dst, recv, d, sem=send):
        return pltpu.make_async_remote_copy(
            src_ref=src, dst_ref=dst, send_sem=sem, recv_sem=recv, device_id={"tp": d}, device_id_type=MESH
        )

    def rows(i):
        return pl.ds(i * SUB, SUB)

    group = (0, 1, 2, 2)
    ag_x = [remote(x_hbm.at[rows(i)], xb.at[BX, rows(i)], ag_recv[g], nx) for i, g in zip((0, 1, 2, 3), group)]
    ag_y = [remote(x_hbm.at[rows(i)], xb.at[BY, rows(i)], ag_recv[g], ny) for i, g in zip((2, 3, 0, 1), group)]
    swap = [
        remote(wg_hbm, w.at[1], swap_recv, sib, swap_send),
        remote(wu_hbm, w.at[3], swap_recv, sib, swap_send),
        remote(wd_hbm, wd.at[pl.ds(half, half)], swap_recv, sib, swap_send),
    ]
    copies = (ag_x, ag_y, swap)

    def start(now):
        for late, _, i in pairs:
            @pl.when(late == now)
            def _():
                for c in copies[i]:
                    c.start()

    start(1)
    local = [
        pltpu.make_async_copy(wg_hbm, w.at[0], w_sem),
        pltpu.make_async_copy(wu_hbm, w.at[2], w_sem),
        pltpu.make_async_copy(wd_hbm, wd.at[pl.ds(0, half)], w_sem),
        pltpu.make_async_copy(x_hbm, xb.at[OWN], w_sem),
    ]
    for c in local:
        c.start()

    @pl.when(first < 3)
    def _():
        pl.semaphore_wait(ready, 3 - first)

    start(0)

    def wait(mib, sem):
        ref = w.at[:, pl.ds(0, int(mib * 2**20) // (4 * 2 * half))]
        pltpu.make_async_copy(ref, ref, sem).wait()

    fw_y = [remote(xb.at[BX, rows(k)], xb.at[BD, rows(2 * k)], fw_recv[k], ny) for k in range(2)]
    fw_x = [remote(xb.at[BY, rows(2 + k)], xb.at[BD, rows(2 * k + 1)], fw_recv[k], nx) for k in range(2)]
    for k in range(2):
        wait((15, 13)[k], ag_recv[k])
        fw_y[k].start()
        fw_x[k].start()

    def unit(b, u, ref, r0):
        x_ref = xb.at[b, pl.ds(u * UNIT, UNIT)]

        def hidden(n, _):
            s, col = n // tiles, pl.ds(pl.multiple_of((n % tiles) * TILE, TILE), TILE)
            gate = jnp.dot(x_ref[...], w[s, :, col], preferred_element_type=F32)
            up = jnp.dot(x_ref[...], w[2 + s, :, col], preferred_element_type=F32)
            hid[:, pl.ds(pl.multiple_of(n * TILE, TILE), TILE)] = (jax.nn.silu(gate) * up).astype(BF16)
            return _

        def down(n, _):
            cols = pl.ds(pl.multiple_of(n * TILE, TILE), TILE)
            v = jnp.dot(hid[...], wd[:, cols], preferred_element_type=F32)
            ref[pl.ds(r0, UNIT), cols] = v.astype(ref.dtype)
            return _

        lax.fori_loop(0, 2 * tiles, hidden, None)
        lax.fori_loop(0, width // TILE, down, None)

    d_x = [remote(pd.at[rows(2 * k)], relx.at[rows(k)], d_recv[k], nx) for k in range(2)]
    d_y = [remote(pd.at[rows(2 * k + 1)], rely.at[rows(k)], d_recv[k], ny) for k in range(2)]
    low, high = pl.ds(0, UNIT), pl.ds(UNIT, UNIT)

    unit(BX, 0, px, 0)
    remote(px, finx.at[low], plain_recv, nx).start()
    unit(BY, 1, py, 0)
    remote(py, finy.at[high], plain_recv, ny).start()
    unit(OWN, 0, own, 0)
    wait(3, ag_recv[2])
    unit(BX, 1, px32, 0)
    unit(BD, 0, pd, 0)
    d_x[0].start()
    d_y[0].start()
    unit(BY, 0, py32, 0)
    wait(1, fw_recv[1])
    unit(BD, 1, pd, UNIT)
    d_x[1].start()
    d_y[1].start()
    unit(OWN, 1, own, UNIT)

    wait(3, d_recv[0])
    own[low] += finx[low].astype(F32)
    own[high] += finy[high].astype(F32)

    def relay(i):
        r0, n, _ = RELAY[i]
        r = pl.ds(r0, n)
        sy[r] = (py32[r] + relx[r].astype(F32)).astype(BF16)
        sx[r] = (px32[r] + rely[r].astype(F32)).astype(BF16)
        sem = lead_send if i == 0 else send
        to_x, to_y = (finx.at[pl.ds(UNIT + r0, n)], finy.at[r]) if i < 3 else (tail_fin.at[1], tail_fin.at[0])
        return remote(sx.at[r], to_x, f_recv[i], nx, sem), remote(sy.at[r], to_y, f_recv[i], ny, sem)

    head, rest = relay(0), relay(1)

    @pl.when(core == 1)
    def _():
        pl.semaphore_wait(turn, 1)

    for c in (*head, *rest):
        c.start()
    wait(12.25, lead_send)

    @pl.when(core == 0)
    def _():
        pl.semaphore_signal(turn, inc=1, device_id={"tp": sib}, device_id_type=MESH)

    wait(1, d_recv[1])
    for i in (2, 3):
        for c in relay(i):
            c.start()

    wait(2 - TAIL / SUB, f_recv[0])
    for u, ref in ((0, finy), (1, finx)):
        r = pl.ds(u * UNIT, UNIT - TAIL)
        out[r] = (own[r] + ref[r].astype(F32)).astype(BF16)
        tail_own[u] = own[pl.ds((u + 1) * UNIT - TAIL, TAIL)]
    wait(TAIL / SUB, f_recv[3])
    wait(11.75, send)


def put(y, tail_own, tail_fin, out, tail, sem):
    step = 8
    for r in range(0, out.shape[0], step):
        if r % UNIT < UNIT - TAIL:
            pltpu.make_async_copy(y.at[pl.ds(r, step)], out.at[pl.ds(r, step)], sem).start()
    tail[...] = (tail_own[...] + tail_fin[...].astype(F32)).astype(BF16)
    for u in range(2):
        pltpu.make_async_copy(tail.at[u], out.at[pl.ds((u + 1) * UNIT - TAIL, TAIL)], sem).start()
    pltpu.make_async_copy(y, y, sem).wait()


def solution(mesh):
    def step(x, w_gate, w_up, w_down):
        rows, depth = x.shape
        half, width = w_down.shape
        vmem = pltpu.VMEM
        dma = pltpu.SemaphoreType.DMA
        flops = 2 * 4 * rows * depth * 2 * half * 3
        parts = pl.pallas_call(
            kernel,
            out_shape=(vmem((rows, width), BF16), vmem((2, TAIL, width), F32), vmem((2, TAIL, width), BF16)),
            in_specs=[pl.BlockSpec(memory_space=pl.ANY)] * 4,
            out_specs=(pl.BlockSpec(memory_space=vmem),) * 3,
            scratch_shapes=[
                vmem((4, depth, half), BF16),
                vmem((2 * half, width), BF16),
                vmem((4, rows, depth), BF16),
                vmem((UNIT, 2 * half), BF16),
                vmem((rows, width), BF16),
                vmem((UNIT, width), BF16),
                vmem((UNIT, width), BF16),
                vmem((UNIT, width), F32),
                vmem((UNIT, width), F32),
                vmem((UNIT, width), BF16),
                vmem((UNIT, width), BF16),
                vmem((rows, width), F32),
                vmem((UNIT, width), BF16),
                vmem((UNIT, width), BF16),
                vmem((rows, width), BF16),
                vmem((rows, width), BF16),
                pltpu.SemaphoreType.REGULAR,
                pltpu.SemaphoreType.REGULAR,
                dma((10,)),
            ],
            compiler_params=pltpu.CompilerParams(
                collective_id=0, has_side_effects=True, vmem_limit_bytes=57 * 2**20
            ),
            cost_estimate=pl.CostEstimate(flops=flops, bytes_accessed=32 * 2**20, transcendentals=0),
            name="mlp",
        )(x, w_gate, w_up, w_down)
        return pl.pallas_call(
            put,
            out_shape=jax.ShapeDtypeStruct((rows, width), BF16),
            in_specs=[pl.BlockSpec(memory_space=vmem)] * 3,
            out_specs=pl.BlockSpec(memory_space=pl.ANY),
            scratch_shapes=[vmem((2, TAIL, width), BF16), dma],
            compiler_params=pltpu.CompilerParams(vmem_limit_bytes=4 * 2**20),
            name="put",
        )(*(pltpu.with_memory_space_constraint(a, vmem) for a in parts))

    return jax.shard_map(
        step,
        mesh=mesh,
        in_specs=(P(("dp", "tp"), None), P(None, "tp"), P(None, "tp"), P("tp", None)),
        out_specs=P(("dp", "tp"), None),
        check_vma=False,
    )
```
